128 devices in a mesh: group: 4 (over y, x), ep: 32 (over z, core).
Axes of the slice: x: 2, y: 2, z: 16, core: 2. Of those that a mesh axis runs over, the one named last changes fastest.
The devices are a block of a 8x8x16 slice.
Arguments:
- tokens: bfloat16 [8192, 3072], P(('group', 'ep')), parts along dimension 0, may hold values from -6 to 6
- expert_ids: int32 [8192, 2], P(('group', 'ep')), parts along dimension 0, may hold values from 0 to 3, all different within a row; in each aligned block of 64 rows (0 to 63, 64 to 127, ...) at most 48 rows name the same one
- w_router: bfloat16 [3072, 4], replicated, may hold values from -0.109375 to 0.109375
- w_gate: bfloat16 [3072, 32768], P(None, 'ep'), may hold values from -0.109375 to 0.109375
- w_up: bfloat16 [3072, 32768], P(None, 'ep'), may hold values from -0.109375 to 0.109375
- w_down: bfloat16 [32768, 3072], P('ep'), may hold values from -0.0625 to 0.0625
- queries: bfloat16 [1024, 24, 128], P(('group', 'ep')), parts along dimension 0, may hold values from -48 to 48
- key_cache: bfloat16 [1024, 256, 4, 128], P(('group', 'ep')), parts along dimension 0, may hold values from -48 to 48
- cached_value_rows: bfloat16 [1024, 256, 4, 128], P(('group', 'ep')), parts along dimension 0, may hold values from -6 to 6
- lengths: int32 [1024], P(('group', 'ep')), parts along dimension 0, may hold values from 2 to 256, as said below
Outputs:
- moe_out: bfloat16 [8192, 3072], P(('group', 'ep')), parts along dimension 0
- attention_out: bfloat16 [1024, 24, 128], P(('group', 'ep')), parts along dimension 0
The draws below stay inside these ranges and needn't reach their ends.
There are 4 independent parts, one for each index of `group`. The reference program is written for one: setup_inputs(seed, part) draws one part's arguments, and reference() takes and returns one part's arrays. A program takes and returns all parts, laid end to end along the dimension named above; an argument that names none is the same for every part. Nothing has to cross between parts.
Inputs may be any that keep to these rules, and one draw needn't show every extreme that they name: `expert_ids`: each row names two different experts; among the rows of one device no expert is named more than 48 times, and some device has an expert named exactly 48 times. `lengths`: every device holds a request of length 256.
All inputs are finite; a program needn't handle non-finite values.
Results may differ from the reference program's by a relative error of at most 0.0085.
Values may be sent and summed in bfloat16 or wider, within the bound.
No kernel may reach another device: no remote copies, remote signals or barrier semaphores. Data moves between devices by JAX's collectives and lax.ppermute only.
A program may use at most 128 MiB of HBM per device.

```python
import math
import jax
import jax.numpy as jnp
import numpy as np
from jax import lax

D = 3072
E = 4
FF = 8192
HEAD_SIZE = 128
KEY_VALUE_HEADS = 4
HQ = 24
TOK_DEV = 64
DEC_DEV = 8
CACHE_POSITIONS = 256
CAP = 48
TP = 8
FF_DEV = 1024
TOKENS = 2048
DECODE_REQUESTS = 256
N_EP = 32


def attention_draw(key):
    base = jax.random.fold_in(key, 4242)
    query_key, cache_random_seed = jax.random.split(base, 2)
    query_draw = jnp.clip(jax.random.normal(query_key, (DECODE_REQUESTS, HQ, HEAD_SIZE), jnp.float32), -6.0, 6.0)
    cache_sample_seed = jnp.clip(jax.random.normal(cache_random_seed, (DECODE_REQUESTS, CACHE_POSITIONS, KEY_VALUE_HEADS, HEAD_SIZE), jnp.float32), -6.0, 6.0)
    return (query_draw, cache_sample_seed)


def draw_queries(key, part):
    return attention_draw(key)[0].astype(jnp.bfloat16)


def draw_key_cache(key, part):
    return attention_draw(key)[1].astype(jnp.bfloat16)


def draw_lengths(key, part):
    base = jax.random.fold_in(key, 77)
    first_key, second_key = jax.random.split(base)
    devices_here = DECODE_REQUESTS // DEC_DEV
    drawn = jax.random.randint(first_key, (devices_here, DEC_DEV), 2, CACHE_POSITIONS + 1, jnp.int32)
    longest = jax.random.randint(second_key, (devices_here, 1), 0, DEC_DEV, jnp.int32)
    filled = jnp.where(jnp.arange(DEC_DEV, dtype=jnp.int32)[None, :] == longest, CACHE_POSITIONS, drawn)
    return filled.reshape(DECODE_REQUESTS)


def block_levels(rng, extent, shards, low, top_value):
    def one(dim, parts):
        heights = jax.random.uniform(jax.random.fold_in(jax.random.fold_in(rng, 6), dim), (parts,), jnp.float32, low / len(shards), top_value / len(shards))
        return jnp.repeat(jnp.exp(heights), extent[dim] // parts).reshape((-1,) + (1,) * (len(extent) - dim - 1))

    level = one(*shards[0])
    for cut in shards[1:]:
        level = level * one(*cut)
    return level


def shared_out(key, own, number, rows, number_of, top, most, slope):
    order = jax.random.permutation(key, number_of)
    packed, usual = load_shares(number_of, rows * top, most, slope, True), load_shares(number_of, rows * top, most, slope, False)
    places = jnp.arange(number_of)

    def named(tallies, rotation):
        used = int((tallies > 0).sum())
        fixed = max(1, used // 4)
        shifted = fixed + (places - fixed + rotation * (used - fixed)) % max(1, number_of - fixed)
        return jnp.zeros((number_of,), jnp.int32).at[order[jnp.where(places < fixed, places, shifted)]].set(jnp.asarray(tallies, jnp.int32))

    tallies = jnp.where(number % 4 == 0, named(packed, number // 4), named(usual, number - number // 4 - 1))
    mixed = jax.random.permutation(jax.random.fold_in(own, 3), number_of)
    donor, taker = mixed[0:number_of // 2 * 2:2], mixed[1:number_of // 2 * 2:2]
    margin = jnp.minimum(tallies[donor] - 1, most - tallies[taker]) // 2
    margin = jnp.where((donor == order[0]) | (taker == order[0]) | (tallies[taker] == 0), 0, jnp.maximum(margin, 0))
    shifted = jax.random.randint(jax.random.fold_in(own, 4), (number_of // 2,), 0, 1 << 20) % (margin + 1)
    tallies = tallies.at[donor].add(-shifted).at[taker].add(shifted)
    items = jnp.searchsorted(jnp.cumsum(tallies), jnp.arange(rows * top), side="right").astype(jnp.int32)
    grid = items.reshape(top, rows).T
    grid = grid[jax.random.permutation(jax.random.fold_in(own, 1), rows)]
    rotation = jax.random.randint(jax.random.fold_in(own, 2), (rows, 1), 0, top)
    return jnp.take_along_axis(grid, (jnp.arange(top)[None, :] + rotation) % top, axis=1)


def load_shares(number_of, total, reach, lean, full):
    loads = [(1 << 20) // math.isqrt(standing ** lean) + 1 for standing in range(1, number_of + 1)]
    largest = reach if full else min(reach, max(-(-total // number_of), total * loads[0] // sum(loads)))
    least = 1 if total - largest >= number_of - 1 else 0
    holding, spare = [largest] + [least] * (number_of - 1), total - largest - least * (number_of - 1)
    while spare > 0:
        movable = [i for i in range(1, number_of) if holding[i] < largest] or [i for i in range(1, number_of) if holding[i] < reach]
        pool, budget = sum([loads[i] for i in movable]), spare
        for i in movable:
            addition = min(reach - holding[i], max(1, budget * loads[i] // pool), spare)
            holding[i] = holding[i] + addition
            spare = spare - addition
    return np.array(holding)


def centred(stream_key, shape, width, reach, cuts=(), kind=jnp.bfloat16):
    result = jax.random.normal(stream_key, shape, jnp.float32) * width
    if len(cuts) > 0:
        result = block_levels(stream_key, shape, cuts, -0.22, 0.18) * result
    return jnp.clip(result, min=-reach, max=reach).astype(kind)


def setup_inputs(seed: int = 0, part: int = 0) -> dict:
    key_list = jax.random.split(jax.random.key(seed), 11)
    own_keys = jax.random.split(jax.random.fold_in(key_list[10], part), 11)
    tokens = centred(own_keys[0], (TOKENS, D), 1.0, 6.0, ((0, 32),))
    expert_ids_keys = jax.random.split(jax.random.fold_in(own_keys[1], 1), TOKENS // TOK_DEV)
    expert_ids_turns = jax.random.permutation(jax.random.fold_in(own_keys[1], 3), TOKENS // TOK_DEV)
    expert_ids = jax.vmap(lambda own, number: shared_out(jax.random.fold_in(own_keys[1], 2), own, number, TOK_DEV, E, 2, CAP, 2))(expert_ids_keys, expert_ids_turns).reshape((TOKENS, 2))
    w_router = centred(key_list[2], (D, E), D ** -0.5, 0.109375)
    w_gate = centred(key_list[3], (D, E * FF), D ** -0.5, 0.109375, ((1, 32),))
    w_up = centred(key_list[4], (D, E * FF), D ** -0.5, 0.109375, ((1, 32),))
    w_down = centred(key_list[5], (E * FF, D), FF ** -0.5, 0.0625, ((0, 32),))
    queries = draw_queries(jax.random.fold_in(jax.random.fold_in(key_list[10], part), 71), part)
    key_cache = draw_key_cache(jax.random.fold_in(jax.random.fold_in(key_list[10], part), 71), part)
    cached_value_rows = centred(own_keys[8], (DECODE_REQUESTS, CACHE_POSITIONS, KEY_VALUE_HEADS, HEAD_SIZE), 1.0, 6.0, ((0, 32),))
    lengths = draw_lengths(jax.random.fold_in(jax.random.fold_in(key_list[10], part), 71), part)
    return {"tokens": tokens, "expert_ids": expert_ids, "w_router": w_router, "w_gate": w_gate, "w_up": w_up, "w_down": w_down, "queries": queries, "key_cache": key_cache, "cached_value_rows": cached_value_rows, "lengths": lengths}


def expert_mlp(inputs, gate_part, up_part, down_part):
    gate_value = jnp.dot(inputs, gate_part, preferred_element_type=jnp.float32)
    up_value = jnp.dot(inputs, up_part, preferred_element_type=jnp.float32)
    hidden = (jax.nn.silu(gate_value) * up_value).astype(jnp.bfloat16)
    row_count = hidden.shape[0]
    split_hidden = hidden.reshape(row_count, TP, FF_DEV).astype(jnp.float32)
    split_down = down_part.reshape(TP, FF_DEV, D).astype(jnp.float32)
    shares = jnp.einsum("rsf,sfd->rsd", split_hidden, split_down, precision=lax.Precision.HIGHEST).astype(jnp.bfloat16)
    shares = lax.optimization_barrier(shares)
    return jnp.sum(shares.astype(jnp.float32), axis=1)


def route_tables(tokens, expert_ids, w_router, capacity):
    token_count = tokens.shape[0]
    expert_count = w_router.shape[1]
    logits = jnp.dot(tokens, w_router, preferred_element_type=jnp.float32)
    labels = jnp.arange(expert_count, dtype=jnp.int32)
    onehot = expert_ids[:, :, None] == labels[None, None, :]
    picked = jnp.sum(jnp.where(onehot, logits[:, None, :], jnp.float32(0.0)), axis=2)
    gate_values = 1.0 / (1.0 + jnp.exp(picked[:, ::-1] - picked))
    flat_hits = onehot.reshape(token_count * 2, expert_count).astype(jnp.int32)
    earlier = jnp.cumsum(flat_hits, axis=0) - flat_hits
    position = jnp.sum(earlier * flat_hits, axis=1).reshape(token_count, 2)
    return gate_values, expert_ids * capacity + position


def decode_attention(queries, key_cache, cached_value_rows, lengths):
    request_count, head_count, head_dim = queries.shape
    cache_len = key_cache.shape[1]
    kv_heads = key_cache.shape[2]
    grouped = queries.reshape(request_count, kv_heads, head_count // kv_heads, head_dim).astype(jnp.float32)
    scores = jnp.einsum("bkgd,blkd->bkgl", grouped, key_cache.astype(jnp.float32), precision=lax.Precision.HIGHEST) * (head_dim ** -0.5)
    visible = jnp.arange(cache_len, dtype=jnp.int32)[None, :] < lengths[:, None]
    scores = jnp.where(visible[:, None, None, :], scores, -jnp.inf)
    row_max = jnp.max(scores, axis=3, keepdims=True)
    exponent = jnp.exp(scores - row_max)
    weights = (exponent / jnp.sum(exponent, axis=3, keepdims=True)).astype(jnp.bfloat16)
    mixed = jnp.einsum("bkgl,blkd->bkgd", weights.astype(jnp.float32), cached_value_rows.astype(jnp.float32), precision=lax.Precision.HIGHEST)
    return mixed.reshape(request_count, head_count, head_dim).astype(jnp.bfloat16)


def reference(tokens, expert_ids, w_router, w_gate, w_up, w_down, queries, key_cache, cached_value_rows, lengths):
    blocks = tokens.reshape(N_EP, TOK_DEV, D)
    block_ids = expert_ids.reshape(N_EP, TOK_DEV, 2)

    def per_source(block_tokens, block_choice):
        return route_tables(block_tokens, block_choice, w_router, CAP)

    gate_values, slot_index = jax.vmap(per_source)(blocks, block_ids)
    position = slot_index - block_ids * CAP
    source = jnp.arange(N_EP, dtype=jnp.int32)[:, None, None] + jnp.zeros((N_EP, TOK_DEV, 2), jnp.int32)
    buffer_row = source * CAP + position
    token_row = source * TOK_DEV + jnp.arange(TOK_DEV, dtype=jnp.int32)[None, :, None]
    table = jnp.full((E, N_EP * CAP), TOKENS, jnp.int32)
    table = table.at[block_ids.reshape(-1), buffer_row.reshape(-1)].set(token_row.reshape(-1))
    padded = jnp.concatenate([tokens, jnp.zeros((1, D), jnp.bfloat16)], axis=0)
    outputs = []
    for expert in range(E):
        inputs = padded[table[expert]]
        outputs.append(expert_mlp(inputs, w_gate[:, expert * FF:(expert + 1) * FF], w_up[:, expert * FF:(expert + 1) * FF], w_down[expert * FF:(expert + 1) * FF, :]))
    stacked = jnp.stack(outputs)
    picked = stacked[block_ids, buffer_row]
    moe_out = jnp.sum(gate_values[..., None] * picked, axis=2).reshape(TOKENS, D).astype(jnp.bfloat16)
    attention_out = decode_attention(queries, key_cache, cached_value_rows, lengths)
    return moe_out, attention_out
```

```python
import functools

import jax
import jax.numpy as jnp
from jax import lax
from jax.experimental import pallas as pl
from jax.experimental.pallas import tpu as pltpu
from jax.sharding import PartitionSpec as P


PAD = 128
VMEM_LIMIT = 8 * 2**20
LOAD_LIMIT = 30 * 2**20
AHEAD = 2


def store_rows(outs, y, gate, cols, segments):
    for index, to, start, count in segments:
        rows = y[start:start + count] * gate[start:start + count]
        outs[index][to:to + count, cols] = rows.astype(jnp.bfloat16)


def row_gates(xs, sel, d):
    return jnp.concatenate([
        jnp.sum(x_ref[:, d:].astype(jnp.float32) * sel[0:1, :], axis=1, keepdims=True)
        for x_ref in xs
    ], axis=0)


def mlp_body(n, outs, segments, up_parts, down_parts, *refs):
    xs = refs[:n]
    sel, wg, wu, wd = refs[n:n + 4]
    ys = refs[n + 4:n + 4 + outs]
    hbuf = refs[n + 4 + outs]
    d, ff = wg.shape
    bh, by = ff // up_parts, d // down_parts

    def up_step(j, carry):
        cols = pl.ds(pl.multiple_of(j * bh, bh), bh)
        x = jnp.concatenate([x_ref[:, :d] for x_ref in xs], axis=0)
        g = jnp.dot(x, wg[:, cols], preferred_element_type=jnp.float32)
        u = jnp.dot(x, wu[:, cols], preferred_element_type=jnp.float32)
        hbuf[:, cols] = (g / (1.0 + jnp.exp(-g)) * u).astype(jnp.bfloat16)
        return carry

    lax.fori_loop(0, up_parts, up_step, 0)
    gate = row_gates(xs, sel, d)

    def down_step(j, carry):
        cols = pl.ds(pl.multiple_of(j * by, by), by)
        y = jnp.dot(hbuf[...], wd[:, cols], preferred_element_type=jnp.float32)
        store_rows(ys, y, gate, cols, segments)
        return carry

    lax.fori_loop(0, down_parts, down_step, 0)


def mlp(xs, sel, wg, wu, wd, out_rows, segments, up_parts=4, down_parts=6):
    d, ff = wg.shape
    n, total = len(xs), sum(x.shape[0] for x in xs)
    vmem = pl.BlockSpec(memory_space=pltpu.VMEM)
    return pl.pallas_call(
        functools.partial(mlp_body, n, len(out_rows), segments, up_parts, down_parts),
        in_specs=[vmem] * (n + 4),
        out_specs=[vmem] * len(out_rows),
        out_shape=[jax.ShapeDtypeStruct((r, d), jnp.bfloat16) for r in out_rows],
        scratch_shapes=[pltpu.VMEM((total, ff), jnp.bfloat16)],
        compiler_params=pltpu.CompilerParams(vmem_limit_bytes=VMEM_LIMIT),
        cost_estimate=pl.CostEstimate(
            flops=6 * total * d * ff, bytes_accessed=6 * d * ff, transcendentals=total * ff
        ),
        name="mlp",
    )(*xs, sel, wg, wu, wd)


def load_body(n, rows, parts, *refs):
    xs = refs[:n]
    sel, wg, wu, wd = refs[n:n + 4]
    ys = refs[n + 4:2 * n + 4]
    gv, uv, dv, hbuf, sg, su, sd = refs[2 * n + 4:]
    d, ff = wg.shape
    bh, by = ff // parts, d // parts
    offs = [sum(rows[:i]) for i in range(n)]

    def up_copies(j):
        cols = pl.ds(pl.multiple_of(j * bh, bh), bh)
        return (
            pltpu.make_async_copy(wg.at[:, cols], gv.at[:, cols], sg.at[j]),
            pltpu.make_async_copy(wu.at[:, cols], uv.at[:, cols], su.at[j]),
        )

    def down_copy(j):
        cols = pl.ds(pl.multiple_of(j * by, by), by)
        return pltpu.make_async_copy(wd.at[:, cols], dv.at[:, cols], sd.at[j])

    def start_up(j):
        for c in up_copies(j):
            c.start()

    for j in range(AHEAD):
        start_up(j)

    def up_step(j, carry):
        for c in up_copies(j):
            c.wait()
        pl.when(j < parts - AHEAD)(lambda: start_up(j + AHEAD))
        pl.when(j >= parts - AHEAD)(lambda: down_copy(j - (parts - AHEAD)).start())
        cols = pl.ds(pl.multiple_of(j * bh, bh), bh)
        x = jnp.concatenate([x_ref[:, :d] for x_ref in xs], axis=0)
        g = jnp.dot(x, gv[:, cols], preferred_element_type=jnp.float32)
        u = jnp.dot(x, uv[:, cols], preferred_element_type=jnp.float32)
        hbuf[:, cols] = (g / (1.0 + jnp.exp(-g)) * u).astype(jnp.bfloat16)
        return carry

    lax.fori_loop(0, parts, up_step, 0)
    gate = row_gates(xs, sel, d)
    segments = tuple((i, 0, off, r) for i, (off, r) in enumerate(zip(offs, rows)))

    def down_step(j, carry):
        down_copy(j).wait()
        pl.when(j < parts - AHEAD)(lambda: down_copy(j + AHEAD).start())
        cols = pl.ds(pl.multiple_of(j * by, by), by)
        y = jnp.dot(hbuf[...], dv[:, cols], preferred_element_type=jnp.float32)
        store_rows(ys, y, gate, cols, segments)
        return carry

    lax.fori_loop(0, parts, down_step, 0)


def load_and_mlp(xs, sel, wg, wu, wd, parts=4):
    d, ff = wg.shape
    rows = tuple(x.shape[0] for x in xs)
    n, total = len(xs), sum(rows)
    vmem = pl.BlockSpec(memory_space=pltpu.VMEM)
    hbm = pl.BlockSpec(memory_space=pltpu.HBM)
    out = pl.pallas_call(
        functools.partial(load_body, n, rows, parts),
        in_specs=[vmem] * (n + 1) + [hbm] * 3,
        out_specs=[vmem] * (n + 3),
        out_shape=[jax.ShapeDtypeStruct((r, d), jnp.bfloat16) for r in rows]
        + [jax.ShapeDtypeStruct(w.shape, w.dtype) for w in (wg, wu, wd)],
        scratch_shapes=[
            pltpu.VMEM((total, ff), jnp.bfloat16),
            pltpu.SemaphoreType.DMA((parts,)),
            pltpu.SemaphoreType.DMA((parts,)),
            pltpu.SemaphoreType.DMA((parts,)),
        ],
        compiler_params=pltpu.CompilerParams(vmem_limit_bytes=LOAD_LIMIT),
        cost_estimate=pl.CostEstimate(
            flops=6 * total * d * ff, bytes_accessed=6 * d * ff, transcendentals=total * ff
        ),
        name="load_and_mlp",
    )(*xs, sel, wg, wu, wd)
    return out[:n], out[n:]


def gate_table(tokens, expert_ids, w_router):
    expert_count = w_router.shape[1]
    logits = jnp.dot(tokens, w_router, preferred_element_type=jnp.float32)
    labels = jnp.arange(expert_count, dtype=jnp.int32)
    onehot = expert_ids[:, :, None] == labels[None, None, :]
    picked = jnp.sum(jnp.where(onehot, logits[:, None, :], jnp.float32(0.0)), axis=2)
    gate_values = 1.0 / (1.0 + jnp.exp(picked[:, ::-1] - picked))
    return jnp.sum(jnp.where(onehot, gate_values[:, :, None], jnp.float32(0.0)), axis=1)


def decode_attention(queries, key_cache, cached_value_rows, lengths):
    request_count, head_count, head_dim = queries.shape
    cache_len = key_cache.shape[1]
    kv_heads = key_cache.shape[2]
    grouped = queries.reshape(request_count, kv_heads, head_count // kv_heads, head_dim)
    scores = jnp.einsum(
        "bkgd,blkd->bkgl", grouped, key_cache, preferred_element_type=jnp.float32
    ) * head_dim ** (-0.5)
    visible = jnp.arange(cache_len, dtype=jnp.int32)[None, :] < lengths[:, None]
    scores = jnp.where(visible[:, None, None, :], scores, -jnp.inf)
    row_max = jnp.max(scores, axis=3, keepdims=True)
    exponent = jnp.exp(scores - row_max)
    weights = (exponent / jnp.sum(exponent, axis=3, keepdims=True)).astype(jnp.bfloat16)
    mixed = jnp.einsum(
        "bkgl,blkd->bkgd", weights, cached_value_rows, preferred_element_type=jnp.float32
    )
    return mixed.reshape(request_count, head_count, head_dim).astype(jnp.bfloat16)


def total_of(*parts):
    acc = parts[0].astype(jnp.float32)
    for p in parts[1:]:
        acc = acc + p.astype(jnp.float32)
    return acc.astype(jnp.bfloat16)


def on_device(
    tokens,
    expert_ids,
    w_router,
    w_gate,
    w_up,
    w_down,
    queries,
    key_cache,
    cached_value_rows,
    lengths,
):
    experts = w_router.shape[1]
    count, _ = tokens.shape
    shards = lax.axis_size("ep")
    chips = shards // 2
    far = chips // 2
    own_expert = lax.axis_index("ep") // (shards // experts)
    out_ring = [(i, (i + (2 if i % 2 == 0 else -2)) % shards) for i in range(shards)]
    back_ring = [(i, (i - (2 if i % 2 == 0 else -2)) % shards) for i in range(shards)]
    half = count // 2
    pair = [(i, i ^ 1) for i in range(shards)]

    def move(v, pairs):
        return lax.ppermute(v, "ep", pairs)

    table = gate_table(tokens, expert_ids, w_router)
    high = lax.reduce_precision(table, 8, 7)
    extra = jnp.concatenate(
        [high, table - high, jnp.zeros((count, PAD - 2 * experts), jnp.float32)], axis=1
    )
    wide = jnp.concatenate([tokens, extra.astype(jnp.bfloat16)], axis=1)
    lanes = jnp.arange(PAD, dtype=jnp.int32)[None, :]
    picks = (lanes == own_expert) | (lanes == own_expert + experts)
    sel = jnp.broadcast_to(picks.astype(jnp.float32), (8, PAD))

    p_in = q_in = wide
    mine_a, mine_b, sib = {}, {}, {}
    held = None
    for step in range(1, far + 2):
        at = step - 1
        p_got, q_got = p_in, q_in
        if step <= far:
            last = step == far
            p_in = move(p_got[:half] if last else p_got, out_ring)
            q_in = move(q_got[half:] if last else q_got, back_ring)
        if at == 0:
            (own, other), held = load_and_mlp(
                [p_got, move(p_got, pair)], sel, w_gate, w_up, w_down
            )
            own_sib = move(other, pair)
            done = (own, other)
        else:
            p_sib, q_sib = move(p_got, pair), move(q_got, pair)
            blocks = [p_got, q_sib, p_sib, q_got]
            n = p_got.shape[0]
            if at == far:
                out_rows = (2 * n, 2 * n)
                segments = ((0, 0, 0, 2 * n), (1, 0, 2 * n, 2 * n))
            else:
                out_rows = (n, n, 2 * n)
                segments = (
                    (0, 0, 0, half), (0, half, n + half, half),
                    (1, 0, half, half), (1, half, n, half),
                    (2, 0, 2 * n, half), (2, half, 3 * n + half, half),
                    (2, n, 2 * n + half, half), (2, n + half, 3 * n, half),
                )
            done = mlp(blocks, sel, *held, out_rows, segments)
            mine_a[at], other = done[0], done[-1]
            if at < far:
                mine_b[at] = done[1]
            sib[at] = move(other, pair)
        if step <= far:
            p_in, q_in, *rest = lax.optimization_barrier((p_in, q_in) + tuple(done))

    first, second = (), ()
    attention_out = None
    for d in range(far - 1, -1, -1):
        if d > 0:
            total = total_of(*second, mine_b[d], sib[d][count:])
            total, sib[d] = lax.optimization_barrier((total, sib[d]))
            if d == 5:
                total, queries = lax.optimization_barrier((total, queries))
                attention_out = decode_attention(queries, key_cache, cached_value_rows, lengths)
            second = (move(total, back_ring),)
        e = d + 1
        total = total_of(*first, mine_a[e], sib[e][:count])
        if d == 2:
            total, attention_out = lax.optimization_barrier((total, attention_out))
        first = (move(total, back_ring),)
    top = move(second[0][half:], pair)
    bottom = move(first[0][half:], pair)
    moe_out = jnp.concatenate([
        total_of(own[:half], own_sib[:half], first[0][:half], top),
        total_of(own[half:], own_sib[half:], second[0][:half], bottom),
    ], axis=0)
    return (moe_out, attention_out)


def solution(mesh):
    in_specs = (
        P(("group", "ep"), None),
        P(("group", "ep"), None),
        P(),
        P(None, "ep"),
        P(None, "ep"),
        P("ep", None),
        P(("group", "ep"), None, None),
        P(("group", "ep"), None, None, None),
        P(("group", "ep"), None, None, None),
        P(("group", "ep")),
    )
    out_specs = (P(("group", "ep"), None), P(("group", "ep"), None, None))

    return jax.shard_map(
        on_device, mesh=mesh, in_specs=in_specs, out_specs=out_specs, check_vma=False
    )
```

```python
import functools

import jax
import jax.numpy as jnp
from jax import lax
from jax.experimental import pallas as pl
from jax.experimental.pallas import tpu as pltpu
from jax.sharding import PartitionSpec as P


PAD = 128
VMEM_LIMIT = 8 * 2**20
LOAD_LIMIT = 30 * 2**20
AHEAD = 3


def store_rows(outs, y, gate, cols, segments):
    for index, to, start, count in segments:
        rows = y[start:start + count] * gate[start:start + count]
        outs[index][to:to + count, cols] = rows.astype(jnp.bfloat16)


def row_gates(xs, sel, d):
    return jnp.concatenate([
        jnp.sum(x_ref[:, d:].astype(jnp.float32) * sel[0:1, :], axis=1, keepdims=True)
        for x_ref in xs
    ], axis=0)


def mlp_body(n, outs, segments, up_parts, down_parts, *refs):
    xs = refs[:n]
    sel, wg, wu, wd = refs[n:n + 4]
    ys = refs[n + 4:n + 4 + outs]
    hbuf = refs[n + 4 + outs]
    d, ff = wg.shape
    bh, by = ff // up_parts, d // down_parts

    def up_step(j, carry):
        cols = pl.ds(pl.multiple_of(j * bh, bh), bh)
        x = jnp.concatenate([x_ref[:, :d] for x_ref in xs], axis=0)
        g = jnp.dot(x, wg[:, cols], preferred_element_type=jnp.float32)
        u = jnp.dot(x, wu[:, cols], preferred_element_type=jnp.float32)
        hbuf[:, cols] = (g / (1.0 + jnp.exp(-g)) * u).astype(jnp.bfloat16)
        return carry

    lax.fori_loop(0, up_parts, up_step, 0)
    gate = row_gates(xs, sel, d)

    def down_step(j, carry):
        cols = pl.ds(pl.multiple_of(j * by, by), by)
        y = jnp.dot(hbuf[...], wd[:, cols], preferred_element_type=jnp.float32)
        store_rows(ys, y, gate, cols, segments)
        return carry

    lax.fori_loop(0, down_parts, down_step, 0)


def mlp(xs, sel, wg, wu, wd, out_rows, segments, up_parts=4, down_parts=6):
    d, ff = wg.shape
    n, total = len(xs), sum(x.shape[0] for x in xs)
    vmem = pl.BlockSpec(memory_space=pltpu.VMEM)
    return pl.pallas_call(
        functools.partial(mlp_body, n, len(out_rows), segments, up_parts, down_parts),
        in_specs=[vmem] * (n + 4),
        out_specs=[vmem] * len(out_rows),
        out_shape=[jax.ShapeDtypeStruct((r, d), jnp.bfloat16) for r in out_rows],
        scratch_shapes=[pltpu.VMEM((total, ff), jnp.bfloat16)],
        compiler_params=pltpu.CompilerParams(vmem_limit_bytes=VMEM_LIMIT),
        cost_estimate=pl.CostEstimate(
            flops=6 * total * d * ff, bytes_accessed=6 * d * ff, transcendentals=total * ff
        ),
        name="mlp",
    )(*xs, sel, wg, wu, wd)


def load_body(n, rows, parts, *refs):
    xs = refs[:n]
    sel, wg, wu, wd = refs[n:n + 4]
    ys = refs[n + 4:2 * n + 4]
    gv, uv, dv, hbuf, sg, su, sd = refs[2 * n + 4:]
    d, ff = wg.shape
    bh, by = ff // parts, d // parts
    offs = [sum(rows[:i]) for i in range(n)]

    def up_copies(j):
        cols = pl.ds(pl.multiple_of(j * bh, bh), bh)
        return (
            pltpu.make_async_copy(wg.at[:, cols], gv.at[:, cols], sg.at[j]),
            pltpu.make_async_copy(wu.at[:, cols], uv.at[:, cols], su.at[j]),
        )

    def down_copy(j):
        cols = pl.ds(pl.multiple_of(j * by, by), by)
        return pltpu.make_async_copy(wd.at[:, cols], dv.at[:, cols], sd.at[j])

    def start_up(j):
        for c in up_copies(j):
            c.start()

    for j in range(AHEAD):
        start_up(j)

    def up_step(j, carry):
        for c in up_copies(j):
            c.wait()
        pl.when(j < parts - AHEAD)(lambda: start_up(j + AHEAD))
        pl.when(j >= parts - AHEAD)(lambda: down_copy(j - (parts - AHEAD)).start())
        cols = pl.ds(pl.multiple_of(j * bh, bh), bh)
        x = jnp.concatenate([x_ref[:, :d] for x_ref in xs], axis=0)
        g = jnp.dot(x, gv[:, cols], preferred_element_type=jnp.float32)
        u = jnp.dot(x, uv[:, cols], preferred_element_type=jnp.float32)
        hbuf[:, cols] = (g / (1.0 + jnp.exp(-g)) * u).astype(jnp.bfloat16)
        return carry

    lax.fori_loop(0, parts, up_step, 0)
    gate = row_gates(xs, sel, d)
    segments = tuple((i, 0, off, r) for i, (off, r) in enumerate(zip(offs, rows)))

    def down_step(j, carry):
        down_copy(j).wait()
        pl.when(j < parts - AHEAD)(lambda: down_copy(j + AHEAD).start())
        cols = pl.ds(pl.multiple_of(j * by, by), by)
        y = jnp.dot(hbuf[...], dv[:, cols], preferred_element_type=jnp.float32)
        store_rows(ys, y, gate, cols, segments)
        return carry

    lax.fori_loop(0, parts, down_step, 0)


def load_and_mlp(xs, sel, wg, wu, wd, parts=4):
    d, ff = wg.shape
    rows = tuple(x.shape[0] for x in xs)
    n, total = len(xs), sum(rows)
    vmem = pl.BlockSpec(memory_space=pltpu.VMEM)
    hbm = pl.BlockSpec(memory_space=pltpu.HBM)
    out = pl.pallas_call(
        functools.partial(load_body, n, rows, parts),
        in_specs=[vmem] * (n + 1) + [hbm] * 3,
        out_specs=[vmem] * (n + 3),
        out_shape=[jax.ShapeDtypeStruct((r, d), jnp.bfloat16) for r in rows]
        + [jax.ShapeDtypeStruct(w.shape, w.dtype) for w in (wg, wu, wd)],
        scratch_shapes=[
            pltpu.VMEM((total, ff), jnp.bfloat16),
            pltpu.SemaphoreType.DMA((parts,)),
            pltpu.SemaphoreType.DMA((parts,)),
            pltpu.SemaphoreType.DMA((parts,)),
        ],
        compiler_params=pltpu.CompilerParams(vmem_limit_bytes=LOAD_LIMIT),
        cost_estimate=pl.CostEstimate(
            flops=6 * total * d * ff, bytes_accessed=6 * d * ff, transcendentals=total * ff
        ),
        name="load_and_mlp",
    )(*xs, sel, wg, wu, wd)
    return out[:n], out[n:]


def gate_table(tokens, expert_ids, w_router):
    expert_count = w_router.shape[1]
    logits = jnp.dot(tokens, w_router, preferred_element_type=jnp.float32)
    labels = jnp.arange(expert_count, dtype=jnp.int32)
    onehot = expert_ids[:, :, None] == labels[None, None, :]
    picked = jnp.sum(jnp.where(onehot, logits[:, None, :], jnp.float32(0.0)), axis=2)
    gate_values = 1.0 / (1.0 + jnp.exp(picked[:, ::-1] - picked))
    return jnp.sum(jnp.where(onehot, gate_values[:, :, None], jnp.float32(0.0)), axis=1)


def attention_weights(queries, key_cache, lengths):
    request_count, head_count, head_dim = queries.shape
    cache_len = key_cache.shape[1]
    kv_heads = key_cache.shape[2]
    grouped = queries.reshape(request_count, kv_heads, head_count // kv_heads, head_dim)
    scores = jnp.einsum(
        "bkgd,blkd->bkgl", grouped, key_cache, preferred_element_type=jnp.float32
    ) * head_dim ** (-0.5)
    visible = jnp.arange(cache_len, dtype=jnp.int32)[None, :] < lengths[:, None]
    scores = jnp.where(visible[:, None, None, :], scores, -jnp.inf)
    row_max = jnp.max(scores, axis=3, keepdims=True)
    exponent = jnp.exp(scores - row_max)
    return (exponent / jnp.sum(exponent, axis=3, keepdims=True)).astype(jnp.bfloat16)


def attention_mix(weights, cached_value_rows):
    mixed = jnp.einsum(
        "bkgl,blkd->bkgd", weights, cached_value_rows, preferred_element_type=jnp.float32
    )
    request_count, kv_heads, group, head_dim = mixed.shape
    return mixed.reshape(request_count, kv_heads * group, head_dim).astype(jnp.bfloat16)


def total_of(*parts):
    acc = parts[0].astype(jnp.float32)
    for p in parts[1:]:
        acc = acc + p.astype(jnp.float32)
    return acc.astype(jnp.bfloat16)


def on_device(
    tokens,
    expert_ids,
    w_router,
    w_gate,
    w_up,
    w_down,
    queries,
    key_cache,
    cached_value_rows,
    lengths,
):
    experts = w_router.shape[1]
    count, _ = tokens.shape
    shards = lax.axis_size("ep")
    chips = shards // 2
    far = chips // 2
    own_expert = lax.axis_index("ep") // (shards // experts)
    out_ring = [(i, (i + (2 if i % 2 == 0 else -2)) % shards) for i in range(shards)]
    back_ring = [(i, (i - (2 if i % 2 == 0 else -2)) % shards) for i in range(shards)]
    half = count // 2
    pair = [(i, i ^ 1) for i in range(shards)]

    def move(v, pairs):
        return lax.ppermute(v, "ep", pairs)

    table = gate_table(tokens, expert_ids, w_router)
    high = lax.reduce_precision(table, 8, 7)
    extra = jnp.concatenate(
        [high, table - high, jnp.zeros((count, PAD - 2 * experts), jnp.float32)], axis=1
    )
    wide = jnp.concatenate([tokens, extra.astype(jnp.bfloat16)], axis=1)
    lanes = jnp.arange(PAD, dtype=jnp.int32)[None, :]
    picks = (lanes == own_expert) | (lanes == own_expert + experts)
    sel = jnp.broadcast_to(picks.astype(jnp.float32), (8, PAD))

    p_in = q_in = wide
    mine_a, mine_b, sib = {}, {}, {}
    held = None
    for step in range(1, far + 2):
        at = step - 1
        p_got, q_got = p_in, q_in
        if step <= far:
            last = step == far
            p_in = move(p_got[:half] if last else p_got, out_ring)
            q_in = move(q_got[half:] if last else q_got, back_ring)
        if at == 0:
            (own, other), held = load_and_mlp(
                [p_got, move(p_got, pair)], sel, w_gate, w_up, w_down
            )
            own_sib = move(other, pair)
            done = (own, other)
        else:
            p_sib, q_sib = move(p_got, pair), move(q_got, pair)
            blocks = [p_got, q_sib, p_sib, q_got]
            n = p_got.shape[0]
            if at == far:
                out_rows = (2 * n, 2 * n)
                segments = ((0, 0, 0, 2 * n), (1, 0, 2 * n, 2 * n))
            else:
                out_rows = (n, n, 2 * n)
                segments = (
                    (0, 0, 0, half), (0, half, n + half, half),
                    (1, 0, half, half), (1, half, n, half),
                    (2, 0, 2 * n, half), (2, half, 3 * n + half, half),
                    (2, n, 2 * n + half, half), (2, n + half, 3 * n, half),
                )
            done = mlp(blocks, sel, *held, out_rows, segments)
            mine_a[at], other = done[0], done[-1]
            if at < far:
                mine_b[at] = done[1]
            sib[at] = move(other, pair)
        if step <= far:
            p_in, q_in, *rest = lax.optimization_barrier((p_in, q_in) + tuple(done))

    own_total = own.astype(jnp.float32) + own_sib.astype(jnp.float32)
    first, second = (), ()
    weights = None
    for d in range(far - 1, -1, -1):
        if d > 0:
            total = total_of(*second, mine_b[d], sib[d][count:])
            total, sib[d] = lax.optimization_barrier((total, sib[d]))
            if d == 2:
                total, own_total = lax.optimization_barrier((total, own_total))
            if d == 1:
                total, queries = lax.optimization_barrier((total, queries))
                weights = attention_weights(queries, key_cache, lengths)
            second = (move(total, back_ring),)
        e = d + 1
        if d == 0:
            *first, weights = lax.optimization_barrier((*first, weights))
        total = total_of(*first, mine_a[e], sib[e][:count])
        first = (move(total, back_ring),)
    attention_out = attention_mix(weights, cached_value_rows)
    *first, attention_out = lax.optimization_barrier((*first, attention_out))
    top = move(second[0][half:], pair)
    bottom = move(first[0][half:], pair)
    moe_out = total_of(
        own_total,
        jnp.concatenate([first[0][:half], second[0][:half]], axis=0),
        jnp.concatenate([top, bottom], axis=0),
    )
    return (moe_out, attention_out)


def solution(mesh):
    in_specs = (
        P(("group", "ep"), None),
        P(("group", "ep"), None),
        P(),
        P(None, "ep"),
        P(None, "ep"),
        P("ep", None),
        P(("group", "ep"), None, None),
        P(("group", "ep"), None, None, None),
        P(("group", "ep"), None, None, None),
        P(("group", "ep")),
    )
    out_specs = (P(("group", "ep"), None), P(("group", "ep"), None, None))

    return jax.shard_map(
        on_device, mesh=mesh, in_specs=in_specs, out_specs=out_specs, check_vma=False
    )
```

```python
import functools

import jax
import jax.numpy as jnp
from jax import lax
from jax.experimental import pallas as pl
from jax.experimental.pallas import tpu as pltpu
from jax.sharding import PartitionSpec as P


PAD = 128
VMEM_LIMIT = 8 * 2**20
LOAD_LIMIT = 30 * 2**20
AHEAD = 3


def store_rows(outs, y, gate, cols, segments):
    for index, to, start, count in segments:
        rows = y[start:start + count] * gate[start:start + count]
        outs[index][to:to + count, cols] = rows.astype(jnp.bfloat16)


def row_gates(xs, sel, d):
    return jnp.concatenate([
        jnp.sum(x_ref[:, d:].astype(jnp.float32) * sel[0:1, :], axis=1, keepdims=True)
        for x_ref in xs
    ], axis=0)


def mlp_body(n, outs, segments, up_parts, down_parts, *refs):
    xs = refs[:n]
    sel, wg, wu, wd = refs[n:n + 4]
    ys = refs[n + 4:n + 4 + outs]
    hbuf = refs[n + 4 + outs]
    d, ff = wg.shape
    bh, by = ff // up_parts, d // down_parts

    def up_step(j, carry):
        cols = pl.ds(pl.multiple_of(j * bh, bh), bh)
        x = jnp.concatenate([x_ref[:, :d] for x_ref in xs], axis=0)
        g = jnp.dot(x, wg[:, cols], preferred_element_type=jnp.float32)
        u = jnp.dot(x, wu[:, cols], preferred_element_type=jnp.float32)
        hbuf[:, cols] = (g / (1.0 + jnp.exp(-g)) * u).astype(jnp.bfloat16)
        return carry

    lax.fori_loop(0, up_parts, up_step, 0)
    gate = row_gates(xs, sel, d)

    def down_step(j, carry):
        cols = pl.ds(pl.multiple_of(j * by, by), by)
        y = jnp.dot(hbuf[...], wd[:, cols], preferred_element_type=jnp.float32)
        store_rows(ys, y, gate, cols, segments)
        return carry

    lax.fori_loop(0, down_parts, down_step, 0)


def mlp(xs, sel, wg, wu, wd, out_rows, segments, up_parts=4, down_parts=4):
    d, ff = wg.shape
    n, total = len(xs), sum(x.shape[0] for x in xs)
    vmem = pl.BlockSpec(memory_space=pltpu.VMEM)
    return pl.pallas_call(
        functools.partial(mlp_body, n, len(out_rows), segments, up_parts, down_parts),
        in_specs=[vmem] * (n + 4),
        out_specs=[vmem] * len(out_rows),
        out_shape=[jax.ShapeDtypeStruct((r, d), jnp.bfloat16) for r in out_rows],
        scratch_shapes=[pltpu.VMEM((total, ff), jnp.bfloat16)],
        compiler_params=pltpu.CompilerParams(vmem_limit_bytes=VMEM_LIMIT),
        cost_estimate=pl.CostEstimate(
            flops=6 * total * d * ff, bytes_accessed=6 * d * ff, transcendentals=total * ff
        ),
        name="mlp",
    )(*xs, sel, wg, wu, wd)


def load_body(n, rows, parts, down_parts, *refs):
    xs = refs[:n]
    sel, wg, wu, wd = refs[n:n + 4]
    ys = refs[n + 4:2 * n + 4]
    gv, uv, dv, hbuf, sg, su, sd = refs[2 * n + 4:]
    d, ff = wg.shape
    bh, by = ff // parts, d // down_parts
    offs = [sum(rows[:i]) for i in range(n)]

    def up_copies(j):
        cols = pl.ds(pl.multiple_of(j * bh, bh), bh)
        return (
            pltpu.make_async_copy(wg.at[:, cols], gv.at[:, cols], sg.at[j]),
            pltpu.make_async_copy(wu.at[:, cols], uv.at[:, cols], su.at[j]),
        )

    def down_copy(j):
        cols = pl.ds(pl.multiple_of(j * by, by), by)
        return pltpu.make_async_copy(wd.at[:, cols], dv.at[:, cols], sd.at[j])

    def start_up(j):
        for c in up_copies(j):
            c.start()

    for j in range(AHEAD):
        start_up(j)

    def up_step(j, carry):
        for c in up_copies(j):
            c.wait()
        pl.when(j < parts - AHEAD)(lambda: start_up(j + AHEAD))
        pl.when(j >= parts - AHEAD)(lambda: down_copy(j - (parts - AHEAD)).start())
        cols = pl.ds(pl.multiple_of(j * bh, bh), bh)
        x = jnp.concatenate([x_ref[:, :d] for x_ref in xs], axis=0)
        g = jnp.dot(x, gv[:, cols], preferred_element_type=jnp.float32)
        u = jnp.dot(x, uv[:, cols], preferred_element_type=jnp.float32)
        hbuf[:, cols] = (g / (1.0 + jnp.exp(-g)) * u).astype(jnp.bfloat16)
        return carry

    lax.fori_loop(0, parts, up_step, 0)
    gate = row_gates(xs, sel, d)
    segments = tuple((i, 0, off, r) for i, (off, r) in enumerate(zip(offs, rows)))

    def down_step(j, carry):
        down_copy(j).wait()
        pl.when(j < down_parts - AHEAD)(lambda: down_copy(j + AHEAD).start())
        cols = pl.ds(pl.multiple_of(j * by, by), by)
        y = jnp.dot(hbuf[...], dv[:, cols], preferred_element_type=jnp.float32)
        store_rows(ys, y, gate, cols, segments)
        return carry

    lax.fori_loop(0, down_parts, down_step, 0)


def load_and_mlp(xs, sel, wg, wu, wd, parts=4, down_parts=4):
    d, ff = wg.shape
    rows = tuple(x.shape[0] for x in xs)
    n, total = len(xs), sum(rows)
    vmem = pl.BlockSpec(memory_space=pltpu.VMEM)
    hbm = pl.BlockSpec(memory_space=pltpu.HBM)
    out = pl.pallas_call(
        functools.partial(load_body, n, rows, parts, down_parts),
        in_specs=[vmem] * (n + 1) + [hbm] * 3,
        out_specs=[vmem] * (n + 3),
        out_shape=[jax.ShapeDtypeStruct((r, d), jnp.bfloat16) for r in rows]
        + [jax.ShapeDtypeStruct(w.shape, w.dtype) for w in (wg, wu, wd)],
        scratch_shapes=[
            pltpu.VMEM((total, ff), jnp.bfloat16),
            pltpu.SemaphoreType.DMA((parts,)),
            pltpu.SemaphoreType.DMA((parts,)),
            pltpu.SemaphoreType.DMA((down_parts,)),
        ],
        compiler_params=pltpu.CompilerParams(vmem_limit_bytes=LOAD_LIMIT),
        cost_estimate=pl.CostEstimate(
            flops=6 * total * d * ff, bytes_accessed=6 * d * ff, transcendentals=total * ff
        ),
        name="load_and_mlp",
    )(*xs, sel, wg, wu, wd)
    return out[:n], out[n:]


def gate_table(tokens, expert_ids, w_router):
    expert_count = w_router.shape[1]
    logits = jnp.dot(tokens, w_router, preferred_element_type=jnp.float32)
    labels = jnp.arange(expert_count, dtype=jnp.int32)[None, :]
    chosen = (expert_ids[:, 0:1] == labels) | (expert_ids[:, 1:2] == labels)
    both = jnp.sum(jnp.where(chosen, logits, jnp.float32(0.0)), axis=1, keepdims=True)
    other = both - logits
    return jnp.where(chosen, 1.0 / (1.0 + jnp.exp(other - logits)), jnp.float32(0.0))


def attention_weights(queries, key_cache, lengths):
    request_count, head_count, head_dim = queries.shape
    cache_len = key_cache.shape[1]
    kv_heads = key_cache.shape[2]
    grouped = queries.reshape(request_count, kv_heads, head_count // kv_heads, head_dim)
    scores = jnp.einsum(
        "bkgd,blkd->bkgl", grouped, key_cache, preferred_element_type=jnp.float32
    ) * head_dim ** (-0.5)
    visible = jnp.arange(cache_len, dtype=jnp.int32)[None, :] < lengths[:, None]
    scores = jnp.where(visible[:, None, None, :], scores, -jnp.inf)
    row_max = jnp.max(scores, axis=3, keepdims=True)
    exponent = jnp.exp(scores - row_max)
    return (exponent / jnp.sum(exponent, axis=3, keepdims=True)).astype(jnp.bfloat16)


def attention_mix(weights, cached_value_rows):
    mixed = jnp.einsum(
        "bkgl,blkd->bkgd", weights, cached_value_rows, preferred_element_type=jnp.float32
    )
    request_count, kv_heads, group, head_dim = mixed.shape
    return mixed.reshape(request_count, kv_heads * group, head_dim).astype(jnp.bfloat16)


def total_of(*parts):
    acc = parts[0].astype(jnp.float32)
    for p in parts[1:]:
        acc = acc + p.astype(jnp.float32)
    return acc.astype(jnp.bfloat16)


def on_device(
    tokens,
    expert_ids,
    w_router,
    w_gate,
    w_up,
    w_down,
    queries,
    key_cache,
    cached_value_rows,
    lengths,
):
    experts = w_router.shape[1]
    count, _ = tokens.shape
    shards = lax.axis_size("ep")
    chips = shards // 2
    far = chips // 2
    own_expert = lax.axis_index("ep") // (shards // experts)
    out_ring = [(i, (i + (2 if i % 2 == 0 else -2)) % shards) for i in range(shards)]
    back_ring = [(i, (i - (2 if i % 2 == 0 else -2)) % shards) for i in range(shards)]
    half = count // 2
    pair = [(i, i ^ 1) for i in range(shards)]

    def move(v, pairs):
        return lax.ppermute(v, "ep", pairs)

    table = gate_table(tokens, expert_ids, w_router)
    high = lax.reduce_precision(table, 8, 7)
    extra = jnp.concatenate(
        [high, table - high, jnp.zeros((count, PAD - 2 * experts), jnp.float32)], axis=1
    )
    wide = jnp.concatenate([tokens, extra.astype(jnp.bfloat16)], axis=1)
    lanes = jnp.arange(PAD, dtype=jnp.int32)[None, :]
    picks = (lanes == own_expert) | (lanes == own_expert + experts)
    sel = jnp.broadcast_to(picks.astype(jnp.float32), (8, PAD))

    p_in = q_in = wide
    mine_a, mine_b, sib = {}, {}, {}
    held = None
    for step in range(1, far + 2):
        at = step - 1
        p_got, q_got = p_in, q_in
        if step <= far:
            last = step == far
            p_in = move(p_got[:half] if last else p_got, out_ring)
            q_in = move(q_got[half:] if last else q_got, back_ring)
        if at == 0:
            (own, other), held = load_and_mlp(
                [p_got, move(p_got, pair)], sel, w_gate, w_up, w_down
            )
            own_sib = move(other, pair)
            done = (own, other)
        else:
            p_sib, q_sib = move(p_got, pair), move(q_got, pair)
            blocks = [p_got, q_sib, p_sib, q_got]
            n = p_got.shape[0]
            if at == far:
                out_rows = (2 * n, 2 * n)
                segments = ((0, 0, 0, 2 * n), (1, 0, 2 * n, 2 * n))
            else:
                out_rows = (n, n, 2 * n)
                segments = (
                    (0, 0, 0, half), (0, half, n + half, half),
                    (1, 0, half, half), (1, half, n, half),
                    (2, 0, 2 * n, half), (2, half, 3 * n + half, half),
                    (2, n, 2 * n + half, half), (2, n + half, 3 * n, half),
                )
            done = mlp(blocks, sel, *held, out_rows, segments)
            mine_a[at], other = done[0], done[-1]
            if at < far:
                mine_b[at] = done[1]
            sib[at] = move(other, pair)
        if step <= far:
            p_in, q_in, *rest = lax.optimization_barrier((p_in, q_in) + tuple(done))

    own_total = own.astype(jnp.float32) + own_sib.astype(jnp.float32)
    first, second = (), ()
    weights = None
    for d in range(far - 1, -1, -1):
        if d > 0:
            total = total_of(*second, mine_b[d], sib[d][count:])
            total, sib[d] = lax.optimization_barrier((total, sib[d]))
            if d == 2:
                total, own_total = lax.optimization_barrier((total, own_total))
            if d == 1:
                total, queries = lax.optimization_barrier((total, queries))
                weights = attention_weights(queries, key_cache, lengths)
            second = (move(total, back_ring),)
        e = d + 1
        if d == 0:
            *first, weights = lax.optimization_barrier((*first, weights))
        total = total_of(*first, mine_a[e], sib[e][:count])
        first = (move(total, back_ring),)
    attention_out = attention_mix(weights, cached_value_rows)
    *first, attention_out = lax.optimization_barrier((*first, attention_out))
    top = move(second[0][half:], pair)
    bottom = move(first[0][half:], pair)
    moe_out = total_of(
        own_total,
        jnp.concatenate([first[0][:half], second[0][:half]], axis=0),
        jnp.concatenate([top, bottom], axis=0),
    )
    return (moe_out, attention_out)


def solution(mesh):
    in_specs = (
        P(("group", "ep"), None),
        P(("group", "ep"), None),
        P(),
        P(None, "ep"),
        P(None, "ep"),
        P("ep", None),
        P(("group", "ep"), None, None),
        P(("group", "ep"), None, None, None),
        P(("group", "ep"), None, None, None),
        P(("group", "ep")),
    )
    out_specs = (P(("group", "ep"), None), P(("group", "ep"), None, None))

    return jax.shard_map(
        on_device, mesh=mesh, in_specs=in_specs, out_specs=out_specs, check_vma=False
    )
```
